32 devices in a mesh: rep: 1 (over z), dp: 32 (over x, y, core).
Axes of the slice: x: 4, y: 4, z: 1, core: 2. Of those that a mesh axis runs over, the one named last changes fastest.
The devices are a block of a 4x4x8 slice.
Arguments:
- x: bfloat16 [32, 1024, 640], P(('rep', 'dp'))
- dy: bfloat16 [32, 1024, 640], P(('rep', 'dp'))
- wq: bfloat16 [2, 640, 512], replicated
- wk: bfloat16 [2, 640, 128], replicated
- wv: bfloat16 [2, 640, 128], replicated
- wo: bfloat16 [2, 512, 640], replicated
- w_gate: bfloat16 [2, 640, 4096], replicated
- w_up: bfloat16 [2, 640, 4096], replicated
- w_down: bfloat16 [2, 4096, 640], replicated
- m_wq: float32 [2, 640, 512], replicated
- m_wk: float32 [2, 640, 128], replicated
- m_wv: float32 [2, 640, 128], replicated
- m_wo: float32 [2, 512, 640], replicated
- m_w_gate: float32 [2, 640, 4096], replicated
- m_w_up: float32 [2, 640, 4096], replicated
- m_w_down: float32 [2, 4096, 640], replicated
- v_wq: float32 [2, 640, 512], replicated
- v_wk: float32 [2, 640, 128], replicated
- v_wv: float32 [2, 640, 128], replicated
- v_wo: float32 [2, 512, 640], replicated
- v_w_gate: float32 [2, 640, 4096], replicated
- v_w_up: float32 [2, 640, 4096], replicated
- v_w_down: float32 [2, 4096, 640], replicated
Outputs:
- output 1: bfloat16 [2, 640, 512], P('rep')
- output 2: bfloat16 [2, 640, 128], P('rep')
- output 3: bfloat16 [2, 640, 128], P('rep')
- output 4: bfloat16 [2, 512, 640], P('rep')
- output 5: bfloat16 [2, 640, 4096], P('rep')
- output 6: bfloat16 [2, 640, 4096], P('rep')
- output 7: bfloat16 [2, 4096, 640], P('rep')
- output 8: float32 [2, 640, 512], P('rep')
- output 9: float32 [2, 640, 128], P('rep')
- output 10: float32 [2, 640, 128], P('rep')
- output 11: float32 [2, 512, 640], P('rep')
- output 12: float32 [2, 640, 4096], P('rep')
- output 13: float32 [2, 640, 4096], P('rep')
- output 14: float32 [2, 4096, 640], P('rep')
- output 15: float32 [2, 640, 512], P('rep')
- output 16: float32 [2, 640, 128], P('rep')
- output 17: float32 [2, 640, 128], P('rep')
- output 18: float32 [2, 512, 640], P('rep')
- output 19: float32 [2, 640, 4096], P('rep')
- output 20: float32 [2, 640, 4096], P('rep')
- output 21: float32 [2, 4096, 640], P('rep')
All inputs are finite; a program needn't handle non-finite values.
Results may differ from the reference program's by a relative error of at most 0.0312.
Values are sent between devices in bfloat16 or wider.
A program may use at most 768 MiB of HBM per device.

```python
import jax
import jax.numpy as jnp
from jax import lax

SEQUENCES = 32
TOKENS = 1024
D = 640
HEADS = 4
KV_HEADS = 1
HEAD = 128
FF = 4096
LAYERS = 2
THETA = 10000
NAMES = ("wq", "wk", "wv", "wo", "w_gate", "w_up", "w_down")
SHAPES = {
    "wq": (LAYERS, D, HEADS * HEAD),
    "wk": (LAYERS, D, KV_HEADS * HEAD),
    "wv": (LAYERS, D, KV_HEADS * HEAD),
    "wo": (LAYERS, HEADS * HEAD, D),
    "w_gate": (LAYERS, D, FF),
    "w_up": (LAYERS, D, FF),
    "w_down": (LAYERS, FF, D),
}


def bump(key, n, height):
    away = (jnp.arange(n, dtype=jnp.int32) - jax.random.randint(key, (), 0, n, jnp.int32)) % n
    return jnp.where(away < n // 8, height, 1.0)


def together(key, own, strength):
    shared = jax.random.normal(key, own.shape[1:], jnp.float32)
    return (own + strength * shared) * lax.rsqrt(1 + strength * strength)


def setup_inputs(seed: int = 0, part: int = 0) -> dict:
    kx, kdy, ka, kb, kz, kf, kh, kl, *keys = jax.random.split(jax.random.key(seed), 8 + 3 * len(NAMES))
    kx, kdy, ka, kb = (jax.random.fold_in(k, part) for k in (kx, kdy, ka, kb))
    kw, km, kv = (keys[i::3] for i in range(3))
    shape = (SEQUENCES, TOKENS, D)
    much_x, much_dy = jax.random.uniform(kz, (2,), jnp.float32, 0.0, 1.0)
    loud = 2.0 ** jax.random.uniform(jax.random.fold_in(kz, 1), (), jnp.float32, -1.0, 2.0)
    layers = 2.0 ** jax.random.uniform(kl, (LAYERS, 1, 1), jnp.float32, -1.0, 1.0)
    times = {"wq": 1.0, "wk": 1.0, "wv": 2.0, "wo": layers, "w_gate": 1.0, "w_up": bump(kh, FF, 4.0), "w_down": layers}
    x = together(ka, jax.random.normal(kx, shape, jnp.float32), much_x) * bump(kf, D, 4.0)
    dy = together(kb, jax.random.normal(kdy, shape, jnp.float32), much_dy)
    drawn = {"x": x.astype(jnp.bfloat16), "dy": (loud * dy * (SEQUENCES * TOKENS) ** -0.5).astype(jnp.bfloat16)}
    for key, name in zip(kw, NAMES, strict=True):
        drawn[name] = (jax.random.normal(key, SHAPES[name], jnp.float32) * SHAPES[name][1] ** -0.5 * times[name]).astype(jnp.bfloat16)
    for key, name in zip(km, NAMES, strict=True):
        drawn[f"m_{name}"] = 0.1 * jax.random.normal(key, SHAPES[name], jnp.float32)
    for key, name in zip(kv, NAMES, strict=True):
        drawn[f"v_{name}"] = jax.random.uniform(key, SHAPES[name], jnp.float32, 0.02, 0.06)
    return drawn


def matmul(a, w):
    return jnp.dot(a, w, preferred_element_type=jnp.float32).astype(jnp.bfloat16)


def normed(h):
    wide = h.astype(jnp.float32)
    scale = lax.rsqrt(jnp.mean(wide**2, -1, keepdims=True) + 1e-6)
    return (wide * scale).astype(jnp.bfloat16)


def turned(t, theta):
    half = t.shape[-1] // 2
    angle = jnp.arange(t.shape[0], dtype=jnp.float32)[:, None] * theta ** (-jnp.arange(half, dtype=jnp.float32) / half)
    cos, sin = jnp.cos(angle)[:, None], jnp.sin(angle)[:, None]
    a, b = t[..., :half].astype(jnp.float32), t[..., half:].astype(jnp.float32)
    return jnp.concatenate([a * cos - b * sin, b * cos + a * sin], -1).astype(jnp.bfloat16)


def seen_by(q, k, v):
    tokens, kv = q.shape[0], k.shape[1]
    q = q.reshape(tokens, kv, -1, q.shape[-1])
    scores = jnp.einsum("tgsd,ugd->gstu", q.astype(jnp.float32), k.astype(jnp.float32)) * q.shape[-1] ** -0.5
    place = jnp.arange(tokens)
    weights = jax.nn.softmax(jnp.where(place[:, None] >= place, scores, -jnp.inf), -1).astype(jnp.bfloat16)
    return jnp.einsum("gstu,ugd->tgsd", weights.astype(jnp.float32), v.astype(jnp.float32)).astype(jnp.bfloat16).reshape(tokens, -1)


def layer(h, w):
    a = normed(h)
    q, k = (turned(matmul(a, w[name]).reshape(h.shape[0], -1, HEAD), THETA) for name in ("wq", "wk"))
    h = h + matmul(seen_by(q, k, matmul(a, w["wv"]).reshape(h.shape[0], -1, HEAD)), w["wo"])
    b = normed(h)
    gate = jnp.dot(b, w["w_gate"], preferred_element_type=jnp.float32)
    up = jnp.dot(b, w["w_up"], preferred_element_type=jnp.float32)
    return h + matmul((jax.nn.silu(gate) * up).astype(jnp.bfloat16), w["w_down"])


def adamw(w, m, v, g):
    m = 0.9 * m + 0.1 * g
    v = 0.95 * v + 0.05 * g * g
    step = m * lax.rsqrt(v + 1e-8) + 0.1 * w
    return (w - 0.02 * step).astype(jnp.bfloat16), m, v


def clipped(gradients, sum_of_squares, count):
    factor = jnp.minimum(1.0, 0.5 * lax.rsqrt(sum_of_squares / count + 1e-30))
    return [g * factor for g in gradients]


def stack(weights, h):
    return lax.scan(lambda h, w: (layer(h, w), None), h, weights)[0]


def reference(x, dy, wq, wk, wv, wo, w_gate, w_up, w_down, m_wq, m_wk, m_wv, m_wo, m_w_gate, m_w_up, m_w_down, v_wq, v_wk, v_wv, v_wo, v_w_gate, v_w_up, v_w_down):
    weights = dict(zip(NAMES, (wq, wk, wv, wo, w_gate, w_up, w_down), strict=True))

    def take(so_far, sequence):
        h, by_y = sequence
        _, back = jax.vjp(stack, weights, h)
        by_weights, by_h = back(by_y)
        return jax.tree.map(lambda total, term: total + term.astype(jnp.float32), so_far, by_weights), by_h

    none_yet = {name: jnp.zeros(w.shape, jnp.float32) for name, w in weights.items()}
    by_weights, by_x = lax.scan(take, none_yet, (x, dy))
    gradients = [by_weights[name].astype(jnp.bfloat16).astype(jnp.float32) for name in NAMES]
    gradients = clipped(gradients, sum(jnp.sum(g * g) for g in gradients), sum(g.size for g in gradients))
    first = (m_wq, m_wk, m_wv, m_wo, m_w_gate, m_w_up, m_w_down)
    second = (v_wq, v_wk, v_wv, v_wo, v_w_gate, v_w_up, v_w_down)
    new = [adamw(weights[name].astype(jnp.float32), m, v, g) for name, m, v, g in zip(NAMES, first, second, gradients, strict=True)]
    return tuple(one[which] for which in range(3) for one in new)
```

```python
import functools
import math

import jax
import jax.numpy as jnp
from jax import lax
from jax.experimental import pallas as pl
from jax.experimental.pallas import tpu as pltpu
from jax.sharding import PartitionSpec as P

F32, BF16 = jnp.float32, jnp.bfloat16
LANES = 128
HEAD = 128
THETA = 10000
PARTS = 2
BQ = 256
LOG2E = 1.4426950408889634
HIDDEN = -1e30
VM = 60 * 2**20


def _nn(a, b):
    return jnp.dot(a, b, preferred_element_type=F32)


def _nt(a, b):
    return lax.dot_general(a, b, (((1,), (1,)), ((), ())), preferred_element_type=F32)


def _whole(*shape):
    return pl.BlockSpec(shape, lambda i: (0,) * len(shape))


def _out(shape, dtype=BF16):
    return jax.ShapeDtypeStruct(shape, dtype)


def _params(*order, **more):
    return pltpu.CompilerParams(dimension_semantics=order or None, vmem_limit_bytes=VM, **more)


HERE = pl.BlockSpec(memory_space=pltpu.VMEM)
ANY = pl.BlockSpec(memory_space=pl.ANY)
ORDER = "arbitrary"
WAYS = (0, 1)
ALL = slice(None)


def _cols(c):
    return slice(c * LANES, (c + 1) * LANES)


def _cost(flops, transcendentals, size):
    return pl.CostEstimate(flops=flops, transcendentals=transcendentals, bytes_accessed=size)


def _peers(n, body, start):
    return lax.fori_loop(1, n, body, start)


def _last():
    return pl.program_id(0) == pl.num_programs(0) - 1


def _norm(h):
    wide = h.astype(F32)
    return wide, lax.rsqrt(jnp.mean(wide * wide, -1, keepdims=True) + 1e-6)


def _norm_back(h, dy, db):
    wide, s = _norm(h)
    dot = jnp.mean(db * wide, -1, keepdims=True)
    return (dy.astype(F32) + s * db - wide * (s * s * s * dot)).astype(BF16)


def _swap(t):
    half = HEAD // 2
    return jnp.concatenate([t[:, half:], t[:, :half]], 1)


def _turn(t, cos, sin):
    t = t.astype(BF16).astype(F32)
    return (t * cos + _swap(t) * sin).astype(BF16)


def _turn_back(t, cos, sin):
    t = t.astype(BF16).astype(F32)
    return (t * cos + _swap(t * sin)).astype(BF16)


def _head(ref, i, rows=ALL):
    return ref[rows, _cols(i)]


def _scores(k, q, at):
    s = _nt(k, q) * (HEAD**-0.5 * LOG2E)
    n = q.shape[0]
    last = s[at:]
    seen = lax.broadcasted_iota(jnp.int32, last.shape, 0) <= lax.broadcasted_iota(jnp.int32, last.shape, 1)
    last = jnp.where(seen, last, HIDDEN)
    return last if at == 0 else jnp.concatenate([s[:at], last], 0)


def _att_fwd(h_ref, wq_ref, wk_ref, wv_ref, wo_ref, cos_ref, sin_ref, y_ref, q_ref, k_ref, v_ref, o_ref, lse_ref):
    cos, sin = cos_ref[...], sin_ref[...]
    wide, s = _norm(h_ref[...])
    a = (wide * s).astype(BF16)
    t, heads = a.shape[0], wq_ref.shape[2] // HEAD
    q = _nn(a, wq_ref[0])
    for i in range(heads):
        q_ref[:, _cols(i)] = _turn(_head(q, i), cos, sin)
    k_ref[...] = _turn(_nn(a, wk_ref[0]), cos, sin)
    v = _nn(a, wv_ref[0]).astype(BF16)
    v_ref[...] = v
    vt = jnp.concatenate([v.T, jnp.ones((16, t), BF16)], 0)
    for at in range(0, t, BQ):
        rows, n = slice(at, at + BQ), at + BQ
        for i in range(heads):
            x = _scores(k_ref[:n, :], _head(q_ref, i, rows), at)
            top = jnp.max(x, 0, keepdims=True)
            p = jnp.exp2(x - top).astype(BF16)
            mix = _nn(vt[:, :n], p)
            total = mix[HEAD : HEAD + 1]
            o_ref[rows, _cols(i)] = (mix[:HEAD] * (1 / total)).T.astype(BF16)
            lse_ref[i : i + 1, rows] = top + jnp.log2(total)
    out = _nn(o_ref[...], wo_ref[0]).astype(BF16)
    y_ref[...] = (h_ref[...].astype(F32) + out.astype(F32)).astype(BF16)


def _att_specs(l, small):
    return [pl.BlockSpec((1, *w.shape[1:]), lambda i: (l, 0, 0)) for w in small]


def att_fwd(h, small, cos, sin, l):
    t, d = h.shape
    wide, narrow = small[0].shape[2], small[1].shape[2]
    heads = wide // HEAD
    shapes = [(t, d), (t, wide), (t, narrow), (t, narrow), (t, wide)]
    return pl.pallas_call(
        _att_fwd, grid=(1,), in_specs=[_whole(t, d), *_att_specs(l, small), _whole(t, HEAD), _whole(t, HEAD)],
        out_specs=[_whole(*s) for s in shapes] + [_whole(heads, t)],
        out_shape=[jax.ShapeDtypeStruct(s, BF16) for s in shapes] + [jax.ShapeDtypeStruct((heads, t), F32)],
        compiler_params=_params(),
        cost_estimate=_cost(4 * t * d * (wide + narrow) + 4 * t * t * wide, t * t * heads, 8 * t * d), name="att_fwd",
    )(h, *small, cos, sin)


def _att_bwd(h_ref, dy_ref, wq_ref, wk_ref, wv_ref, wo_ref, cos_ref, sin_ref, q_ref, k_ref, v_ref, o_ref, lse_ref, dh_ref, g_ref, do_s, dq_s, dk_s, dv_s):
    cos, sin, dy = cos_ref[...], sin_ref[...], dy_ref[...]
    t, heads = dy.shape[0], wq_ref.shape[2] // HEAD
    do_s[...] = _nt(dy, wo_ref[0]).astype(BF16)
    dot = _nt(wo_ref[0], dy).astype(BF16).astype(F32)
    ot = o_ref[...].T
    both = dot * ot.astype(F32)
    deltas = [jnp.sum(both[_cols(i)], 0, keepdims=True) for i in range(heads)]
    at = 0

    def put(g):
        nonlocal at
        g = g.astype(BF16)
        for c in range(0, g.shape[1], LANES):
            g_ref[at : at + g.shape[0], :] = g[:, c : c + LANES]
            at += g.shape[0]

    g_wo = _nn(ot, dy)
    kt = k_ref[...].T
    dk_s[...] = jnp.zeros_like(dk_s)
    dv_s[...] = jnp.zeros_like(dv_s)
    for first in range(0, t, BQ):
        rows, n = slice(first, first + BQ), first + BQ
        for i in range(heads):
            q, do = _head(q_ref, i, rows), _head(do_s, i, rows)
            p = jnp.exp2(_scores(k_ref[:n, :], q, first) - lse_ref[i : i + 1, rows])
            ds = (p * (_nt(v_ref[:n, :], do) - deltas[i][:, rows])).astype(BF16)
            dv_s[:n, :] += _nn(p.astype(BF16), do)
            dk_s[:n, :] += _nn(ds, q)
            dq = (_nn(kt[:, :n], ds) * HEAD**-0.5).T
            dq_s[rows, _cols(i)] = _turn_back(dq, cos[rows], sin[rows])
    dk = _turn_back(dk_s[...] * HEAD**-0.5, cos, sin)
    dv, dq = dv_s[...].astype(BF16), dq_s[...]
    wide, s = _norm(h_ref[...])
    a_t = (wide * s).astype(BF16).T
    put(_nn(a_t, dq))
    put(_nn(a_t, dk))
    put(_nn(a_t, dv))
    put(g_wo)
    da = _nt(dq, wq_ref[0]) + _nt(dk, wk_ref[0]) + _nt(dv, wv_ref[0])
    dh_ref[...] = _norm_back(h_ref[...], dy, da)


def att_bwd(h, dy, small, cos, sin, kept, l):
    t, d = h.shape
    wide, narrow = small[0].shape[2], small[1].shape[2]
    rows = sum(w[0].size for w in small) // LANES
    return pl.pallas_call(
        _att_bwd, grid=(1,),
        in_specs=[_whole(t, d), _whole(t, d), *_att_specs(l, small), _whole(t, HEAD), _whole(t, HEAD), *(_whole(*a.shape) for a in kept)],
        out_specs=[_whole(t, d), _whole(rows, LANES)],
        out_shape=[jax.ShapeDtypeStruct((t, d), BF16), jax.ShapeDtypeStruct((rows, LANES), BF16)],
        scratch_shapes=[pltpu.VMEM((t, wide), BF16), pltpu.VMEM((t, wide), BF16), pltpu.VMEM((t, narrow), F32), pltpu.VMEM((t, narrow), F32)],
        compiler_params=_params(),
        cost_estimate=_cost(8 * t * d * (wide + narrow) + 10 * t * t * wide, t * t * wide // HEAD, 12 * t * d), name="att_bwd",
    )(h, dy, *small, cos, sin, *kept)


def _ffn_fwd(h_ref, wg_ref, wu_ref, wd_ref, y_ref, *rest, keep):
    (g_ref, u_ref) = rest[:2] if keep else (None, None)
    b_s, y_s = rest[-2:]
    i = pl.program_id(0)
    @pl.when(i == 0)
    def _():
        wide, s = _norm(h_ref[...])
        b_s[...] = (wide * s).astype(BF16)
        y_s[...] = jnp.zeros_like(y_s)
    b = b_s[...]
    gate = _nn(b, wg_ref[0])
    up = _nn(b, wu_ref[0])
    if keep:
        g_ref[...] = gate
        u_ref[...] = up
    hid = (gate * (1 / (1 + jnp.exp(-gate))) * up).astype(BF16)
    y_s[...] += _nn(hid, wd_ref[0])
    @pl.when(_last())
    def _():
        y_ref[...] = (h_ref[...].astype(F32) + y_s[...].astype(BF16).astype(F32)).astype(BF16)

def ffn_fwd(h, wg, wu, wd, l, fc=512, keep=True):
    t, d = h.shape
    ff = wg.shape[2]
    whole = _whole(t, d)
    outs = [jax.ShapeDtypeStruct((t, d), BF16)]
    ospecs = [whole]
    if keep:
        outs += [jax.ShapeDtypeStruct((t, ff), F32)] * 2
        ospecs += [pl.BlockSpec((t, fc), lambda i: (0, i))] * 2
    return pl.pallas_call(
        functools.partial(_ffn_fwd, keep=keep), grid=(ff // fc,),
        in_specs=[whole, pl.BlockSpec((1, d, fc), lambda i: (l, 0, i)), pl.BlockSpec((1, d, fc), lambda i: (l, 0, i)),
                  pl.BlockSpec((1, fc, d), lambda i: (l, i, 0))],
        out_specs=ospecs, out_shape=outs,
        scratch_shapes=[pltpu.VMEM((t, d), BF16), pltpu.VMEM((t, d), F32)],
        compiler_params=_params(ORDER),
        cost_estimate=_cost(6 * t * d * ff, t * ff, 3 * d * ff * 2), name="ffn_fwd",
    )(h, wg, wu, wd)

def _ffn_bwd(*refs, saved, first, last):
    refs = list(refs)
    h_ref, dy_ref, wg_ref, wu_ref, wd_ref = refs[:5]
    refs = refs[5:]
    if saved:
        g_ref, u_ref = refs[:2]
        refs = refs[2:]
    if not first:
        db_in = refs.pop(0)
    G_ref, db_ref, b_s, bT_s, dyT_s, db_s = refs
    i = pl.program_id(0)
    @pl.when(i == 0)
    def _():
        wide, s = _norm(h_ref[...])
        b = (wide * s).astype(BF16)
        b_s[...] = b
        bT_s[...] = b.T
        dyT_s[...] = dy_ref[...].T
        db_s[...] = jnp.zeros_like(db_s) if first else db_in[...]
    b, dy = b_s[...], dy_ref[...]
    wg, wu, wd = wg_ref[0], wu_ref[0], wd_ref[0]
    fc = wg.shape[1]
    if saved:
        gate, up = g_ref[...], u_ref[...]
    else:
        gate, up = _nn(b, wg), _nn(b, wu)
    dhid = _nt(dy, wd).astype(BF16).astype(F32)
    sig = 1 / (1 + jnp.exp(-gate))
    act = gate * sig
    hid = (act * up).astype(BF16)
    dup = (dhid * act).astype(BF16)
    dgate = (dhid * up * (sig * (1 + gate * (1 - sig)))).astype(BF16)
    db_s[...] += _nt(dgate, wg) + _nt(dup, wu)
    bT, dyT = bT_s[...], dyT_s[...]
    for k, (x, z) in enumerate(((bT, dgate), (bT, dup), (dyT, hid))):
        w = _nn(x, z).astype(BF16)
        for c in range(fc // LANES):
            G_ref[c, k] = w[:, _cols(c)]
    @pl.when(_last())
    def _():
        if not last:
            db_ref[...] = db_s[...]
        else:
            db_ref[...] = _norm_back(h_ref[...], dy_ref[...], db_s[...])

def ffn_bwd(h, dy, wg, wu, wd, l, part, parts, fc=512, kept=None, db_in=None):
    t, d = h.shape
    ff = wg.shape[2]
    n = ff // parts // fc
    o = part * n
    first, last = part == 0, part == parts - 1
    whole = _whole(t, d)
    col = pl.BlockSpec((1, d, fc), lambda i: (l, 0, i + o))
    args, specs = [h, dy, wg, wu, wd], [whole, whole, col, col, pl.BlockSpec((1, fc, d), lambda i: (l, i + o, 0))]
    if kept is not None:
        args += list(kept)
        specs += [pl.BlockSpec((t, fc), lambda i: (0, i + o))] * 2
    if not first:
        args += [db_in]
        specs += [whole]
    return pl.pallas_call(
        functools.partial(_ffn_bwd, saved=kept is not None, first=first, last=last), grid=(n,),
        in_specs=specs,
        out_specs=[pl.BlockSpec((fc // LANES, 3, d, LANES), lambda i: (i, 0, 0, 0)), whole],
        out_shape=[jax.ShapeDtypeStruct((ff // parts // LANES, 3, d, LANES), BF16), jax.ShapeDtypeStruct((t, d), BF16 if last else F32)],
        scratch_shapes=[pltpu.VMEM((t, d), BF16), pltpu.VMEM((d, t), BF16), pltpu.VMEM((d, t), BF16), pltpu.VMEM((t, d), F32)],
        compiler_params=_params(ORDER),
        cost_estimate=_cost(16 * t * d * ff // parts, t * ff // parts, 6 * d * ff * 2 // parts), name="ffn_bwd",
    )(*args)


def _adam(w, m, v, g):
    m = 0.9 * m + 0.1 * g
    v = 0.95 * v + 0.05 * g * g
    return (w.astype(F32) - 0.02 * (m * lax.rsqrt(v + 1e-8) + 0.1 * w.astype(F32))).astype(BF16), m, v


def _ffn_adam(f_ref, g_ref, *refs):
    ins, outs = refs[:9], refs[-9:]
    f = f_ref[0:1, 0:1]
    d, cb = ins[0].shape[1], ins[0].shape[2] // LANES
    for c in range(cb):
        at = _cols(c)
        rows = g_ref[c].reshape(3 * d, LANES)
        for k in range(3):
            g = rows[k * d : (k + 1) * d].astype(F32) * f
            where = (0, ALL, at)
            if k == 2:
                g, where = g.T, (0, at, ALL)
            got = _adam(*(r[where] for r in ins[3 * k : 3 * k + 3]), g)
            for r, x in zip(outs[3 * k : 3 * k + 3], got):
                r[where] = x


def ffn_adam(f, g, block, index, arrays, l, part, parts, so_far, cb=2):
    _, d, ff = arrays[0].shape
    steps = ff // parts // LANES // cb
    wide = pl.BlockSpec((1, d, cb * LANES), lambda i: (l, 0, i + part * steps))
    tall = pl.BlockSpec((1, cb * LANES, d), lambda i: (l, i + part * steps, 0))
    specs = [wide] * 6 + [tall] * 3
    chain = [] if so_far is None else list(so_far)
    return pl.pallas_call(
        _ffn_adam, grid=(steps,),
        in_specs=[_whole(*f.shape), pl.BlockSpec(block, index)] + specs
        + [ANY] * len(chain),
        out_specs=specs, out_shape=[jax.ShapeDtypeStruct(a.shape, a.dtype) for a in arrays],
        input_output_aliases={11 + i: i for i in range(len(chain))},
        compiler_params=_params(ORDER),
        cost_estimate=_cost(6000 * d * ff // parts, 3 * d * ff // parts, 66 * d * ff // parts), name="ffn_adam",
    )(f, g, *arrays, *chain)


def _small_adam(f_ref, g_ref, *refs):
    ins, outs = refs[: len(refs) // 2], refs[len(refs) // 2 :]
    f, at = f_ref[0:1, 0:1], 0
    for k in range(len(ins) // 3):
        _, rows, cols = ins[3 * k].shape
        for c in range(cols // LANES):
            where = (0, ALL, _cols(c))
            g = g_ref[0, at : at + rows].astype(F32) * f
            at += rows
            got = _adam(*(r[where] for r in ins[3 * k : 3 * k + 3]), g)
            for r, x in zip(outs[3 * k : 3 * k + 3], got):
                r[where] = x


def small_adam(f, g, arrays):
    specs = [pl.BlockSpec((1, *a.shape[1:]), lambda i: (i, 0, 0)) for a in arrays]
    return pl.pallas_call(
        _small_adam, grid=(g.shape[0],),
        in_specs=[_whole(*f.shape), pl.BlockSpec((1, *g.shape[1:]), lambda i: (i, 0, 0))] + specs,
        out_specs=specs, out_shape=[jax.ShapeDtypeStruct(a.shape, a.dtype) for a in arrays],
        compiler_params=_params(ORDER),
        cost_estimate=_cost(2000 * g.size, g.size, 22 * g.size), name="small_adam",
    )(f, g, *arrays)


def _factor(x_ref, f_ref, all_s, send, recv, *, axis, n, count):
    me = lax.axis_index(axis)
    barrier = pltpu.get_barrier_semaphore()

    def peer(i):
        return lax.rem(me + i, n)

    def greet(i, _):
        pl.semaphore_signal(barrier, inc=1, device_id={axis: peer(i)}, device_id_type=pl.DeviceIdType.MESH)

    _peers(n, greet, None)
    pl.semaphore_wait(barrier, n - 1)

    def copy(i):
        return pltpu.make_async_remote_copy(src_ref=x_ref, dst_ref=all_s.at[i], send_sem=send.at[i], recv_sem=recv.at[i],
                                            device_id={axis: peer(i)}, device_id_type=pl.DeviceIdType.MESH)

    _peers(n, lambda i, _: copy(i).start(), None)
    _peers(n, lambda i, _: copy(i).wait(), None)
    total = x_ref[...]
    total = _peers(n, lambda i, t: t + all_s[i], total)
    total = jnp.sum(jnp.sum(total, 0, keepdims=True), 1, keepdims=True)
    f_ref[...] = jnp.broadcast_to(jnp.minimum(1.0, 0.5 * lax.rsqrt(total / count + 1e-30)), f_ref.shape)


def factor(x, axis, n, count):
    return pl.pallas_call(
        functools.partial(_factor, axis=axis, n=n, count=count),
        in_specs=[HERE], out_specs=HERE,
        out_shape=jax.ShapeDtypeStruct(x.shape, F32),
        scratch_shapes=[pltpu.VMEM((n, *x.shape), F32), pltpu.SemaphoreType.DMA((n,)), pltpu.SemaphoreType.DMA((n,))],
        compiler_params=pltpu.CompilerParams(collective_id=0, has_side_effects=True),
        cost_estimate=_cost(10**7, 0, 10**6), name="factor",
    )(x)


def _scatter(*refs, axis, rows, side):
    units, (out_ref, *rest) = refs[: len(rows)], refs[len(rows) :]
    bufs, sems = rest[: 9 * len(rows)], rest[9 * len(rows) :]
    own_sem, p0s, p0r, s1s, s1r, s2s, s2r, t1s, t1r, t2s, t2r = sems
    me = lax.axis_index(axis)
    core, x, y = lax.rem(me, 2), lax.div(me, 2 * side), lax.rem(lax.div(me, 2), side)
    device = lambda x, y, core: {axis: (x * side + y) * 2 + core}
    ring = lambda n: lax.rem(n + 2 * side, side)
    partner = device(x, y, 1 - core)
    near = [[device(ring(x + 1), y, core), device(ring(x - 1), y, core)], [device(x, ring(y + 1), core), device(x, ring(y - 1), core)]]
    barrier = pltpu.get_barrier_semaphore()
    for to in [partner, *near[0], *near[1]]:
        pl.semaphore_signal(barrier, inc=1, device_id=to, device_id_type=pl.DeviceIdType.MESH)
    pl.semaphore_wait(barrier, 5)
    flows = [(u, p) for u in range(len(rows)) for p in WAYS]
    left_over = []
    piece_of, chunk_of = (lambda u: rows[u] // 64), (lambda u: rows[u] // 16)

    def send(src, dst, s, r, to):
        copy = pltpu.make_async_remote_copy(src_ref=src, dst_ref=dst, send_sem=s, recv_sem=r, device_id=to, device_id_type=pl.DeviceIdType.MESH)
        copy.start()
        left_over.append(copy)

    def add(n, outs, *ins):
        step = max(b for b in (256, 240, 128, 112, 64) if n % b == 0)

        def body(i, _):
            total = None
            for ref, at in ins:
                t = ref[pl.ds(pl.multiple_of(at + i * step, 16), step), :].astype(F32)
                total = t if total is None else total + t
            for ref, at in outs:
                ref[pl.ds(pl.multiple_of(at + i * step, 16), step), :] = total.astype(ref.dtype)

        lax.fori_loop(0, n // step, body, None)

    own = lambda u: bufs[9 * u]
    other = lambda u: bufs[9 * u + 1]
    (A1, R1, A2, R2, MID, B1, Q1) = (lambda u, i=i: bufs[9 * u + 2 + i] for i in range(7))
    place = lambda p: (x, y)[p]
    cross = lambda p: (y, x)[p]
    chunk = lambda u, p, j: p * (rows[u] // 4) + j * (chunk_of(u))

    def fetch(u, p, j, half):
        piece, base = piece_of(u), half * (rows[u] // 2) + p * (rows[u] // 4)
        if p == 0:
            return [(base + j * (chunk_of(u)), chunk(u, p, j), chunk_of(u))]
        return [(base + (i * side + j) * piece, chunk(u, p, j) + i * piece, piece) for i in range(side)]

    al = lambda n: pl.multiple_of(n, 16)
    at_of = lambda ref, a, n: ref.at[pl.ds(al(a), n), :]
    for f, (u, p) in enumerate(flows):
        for k in (2, 1, 3, 0):
            j = ring(place(p) + k)
            for src, dst, n in fetch(u, p, j, 1 - core):
                copy = pltpu.make_async_remote_copy(src_ref=at_of(units[u], src, n), dst_ref=at_of(other(u), dst, n), send_sem=p0s.at[f, k],
                                                    recv_sem=p0r.at[f, k], device_id=partner, device_id_type=pl.DeviceIdType.MESH)
                copy.start()
            for src, dst, n in fetch(u, p, j, core):
                pltpu.make_async_copy(at_of(units[u], src, n), at_of(own(u), dst, n), own_sem.at[f, k]).start()

    def arrived(f, k):
        u, p = flows[f]
        a, n = chunk(u, p, ring(place(p) + k)), chunk_of(u)
        pltpu.make_async_copy(at_of(own(u), a, n), at_of(own(u), a, n), own_sem.at[f, k]).wait()
        pltpu.make_async_remote_copy(src_ref=at_of(other(u), a, n), dst_ref=at_of(other(u), a, n), send_sem=p0s.at[f, k], recv_sem=p0r.at[f, k],
                                     device_id=partner, device_id_type=pl.DeviceIdType.MESH).wait()
        return a

    def landed(ref, a, n, f, i, sem_s, sem_r, to):
        pltpu.make_async_remote_copy(src_ref=ref.at[pl.ds(a, n), :], dst_ref=ref.at[pl.ds(a, n), :], send_sem=sem_s.at[f, i], recv_sem=sem_r.at[f, i],
                                     device_id=to, device_id_type=pl.DeviceIdType.MESH).wait_recv()

    def one(f):
        u, p = flows[f]
        n = chunk_of(u) // 2
        a = arrived(f, 2)
        add(2 * n, [(A1(u), 2 * p * n)], (own(u), a), (other(u), a))
        for way in WAYS:
            at = (2 * p + way) * n
            send(A1(u).at[pl.ds(at, n), :], R1(u).at[pl.ds(at, n), :], s1s.at[f, way], s1r.at[f, way], near[p][way])

    def two(f):
        u, p = flows[f]
        n = chunk_of(u) // 2
        for way in WAYS:
            a = arrived(f, (1, 3)[way])
            landed(R1(u), (2 * p + way) * n, n, f, way, s1s, s1r, near[p][way])
            at = (2 * p + way) * 2 * n
            with_, plain = way * n, (1 - way) * n
            add(n, [(A2(u), at + with_)], (own(u), a + with_), (other(u), a + with_), (R1(u), (2 * p + way) * n))
            add(n, [(A2(u), at + plain)], (own(u), a + plain), (other(u), a + plain))
            send(A2(u).at[pl.ds(at, 2 * n), :], R2(u).at[pl.ds(at, 2 * n), :], s2s.at[f, way], s2r.at[f, way], near[p][way])

    def three(f):
        u, p = flows[f]
        n, piece = chunk_of(u), piece_of(u)
        a = arrived(f, 0)
        for way in WAYS:
            landed(R2(u), (2 * p + way) * n, n, f, way, s2s, s2r, near[p][way])
        add(n, [(MID(u), p * n)], (own(u), a), (other(u), a), (R2(u), 2 * p * n), (R2(u), (2 * p + 1) * n))
        far = p * n + ring(cross(p) + 2) * piece
        at = p * 3 * piece
        add(piece, [(B1(u), at)], (MID(u), far))
        for way in WAYS:
            here = pl.ds(at + way * (piece // 2), piece // 2)
            send(B1(u).at[here, :], Q1(u).at[here, :], t1s.at[f, way], t1r.at[f, way], near[1 - p][way])

    def four(f):
        u, p = flows[f]
        n, piece = chunk_of(u), piece_of(u)
        for way in WAYS:
            first = 3 * p * piece
            landed(Q1(u), first + way * (piece // 2), piece // 2, f, way, t1s, t1r, near[1 - p][way])
            src = p * n + ring(cross(p) + (1, 3)[way]) * piece
            at = first + (1 + way) * piece
            with_, plain = way * (piece // 2), (1 - way) * (piece // 2)
            add(piece // 2, [(B1(u), at + with_)], (MID(u), src + with_), (Q1(u), first + way * (piece // 2)))
            add(piece // 2, [(B1(u), at + plain)], (MID(u), src + plain))
            send(B1(u).at[pl.ds(at, piece), :], Q1(u).at[pl.ds(at, piece), :], t2s.at[f, way], t2r.at[f, way], near[1 - p][way])

    def five(f):
        u, p = flows[f]
        n, piece = chunk_of(u), piece_of(u)
        first = 3 * p * piece
        for way in WAYS:
            landed(Q1(u), first + (1 + way) * piece, piece, f, way, t2s, t2r, near[1 - p][way])
        add(piece, [(out_ref, sum(r // 32 for r in rows[:u]) + p * piece)], (MID(u), p * n + ring(cross(p)) * piece),
            (Q1(u), first + piece), (Q1(u), first + 2 * piece))

    stages = (one, two, three, four, five)
    for t in range(len(flows) + 2 * (len(stages) - 1)):
        for k, stage in enumerate(stages):
            if 0 <= t - 2 * k < len(flows):
                stage(t - 2 * k)
    for copy in left_over:
        copy.wait_send()


def ring_scatter(units, axis, side):
    rows = tuple(u.shape[0] for u in units)
    buf = lambda n, t=BF16: pltpu.VMEM((n, LANES), t)
    scratch = []
    for r in rows:
        scratch += [buf(r // 2), buf(r // 2), buf(r // 8), buf(r // 8), buf(r // 4), buf(r // 4), buf(r // 8, F32), buf(3 * r // 32), buf(3 * r // 32)]
    f = 2 * len(rows)
    total = sum(rows)
    return pl.pallas_call(
        functools.partial(_scatter, axis=axis, rows=rows, side=side),
        in_specs=[ANY] * len(units), out_specs=HERE,
        out_shape=jax.ShapeDtypeStruct((total // 32, LANES), BF16),
        scratch_shapes=scratch + [pltpu.SemaphoreType.DMA((f, 4))] * 3 + [pltpu.SemaphoreType.DMA((f, 2))] * 8,
        compiler_params=_params(collective_id=1, has_side_effects=True),
        cost_estimate=_cost(5 * 10**10, 0, total * LANES * 2), name="ring_scatter",
    )(*units)


def solution(mesh):
    n = mesh.shape["dp"]

    def step(x, dy, *arrays):
        weights, m, v = (arrays[i : i + 7] for i in (0, 7, 14))
        layers, d, ff = weights[4].shape
        small, (wg, wu, wd) = weights[:4], weights[4:]
        count = sum(w.size for w in weights)
        h = x[0]
        half = HEAD // 2
        angle = jnp.arange(h.shape[0], dtype=F32)[:, None] * THETA ** (-jnp.arange(half, dtype=F32) / half)
        cos, sin = jnp.cos(angle), jnp.sin(angle)
        cos, sin = jnp.concatenate([cos, cos], 1), jnp.concatenate([-sin, sin], 1)
        kept, backs = [], []
        for l in range(layers):
            y, *rest = att_fwd(h, small, cos, sin, l)
            backs.append((h, rest))
            h = y
            if l < layers - 1:
                y, *gu = ffn_fwd(h, wg, wu, wd, l)
                kept.append((h, gu))
                h = y
            else:
                kept.append((h, None))
        by_h = dy[0]
        flat = lambda g: g.reshape(-1, LANES)
        side = math.isqrt(n // 2)
        summed, little = {}, {}
        add_up = lambda s: jnp.sum(jnp.square(s.astype(F32)).reshape(-1, 8, LANES), 0)
        for l in reversed(range(layers)):
            h, gu = kept[l]
            got, units = None, []
            for part in range(PARTS):
                g, got = ffn_bwd(h, by_h, wg, wu, wd, l, part, PARTS, kept=gu, db_in=got)
                units.append(flat(g))
            before, rest = backs[l]
            by_h, little[l] = att_bwd(before, got, small, cos, sin, rest, l)
            if l:
                summed[l] = lax.psum(units, "dp")
        own = jnp.concatenate([little[l] for l in range(layers)])
        little_rows = own.shape[0]
        units.append(jnp.pad(own, ((0, -little_rows % 2048), (0, 0))))
        shard = ring_scatter(units, "dp", side)
        me = lax.axis_index("dp")
        squares = add_up(shard)
        for l in range(1, layers):
            for s in summed[l]:
                rows = s.shape[0] // n
                squares += add_up(lax.dynamic_slice_in_dim(s, me * rows, rows))
        f = factor(squares, "dp", n, count)
        rows = [u.shape[0] // 64 for u in units]
        all_of_0 = lax.all_gather(shard, "dp", axis=0, tiled=True).reshape(side, side, 2, -1, LANES)
        ffn = [a for i in (4, 5, 6) for a in (weights[i], m[i], v[i])]
        so_far, cb = None, 2
        cols = ff // PARTS // LANES // cb
        for l in reversed(range(layers)):
            for part in range(PARTS):
                if l:
                    g, block, index = summed[l][part].reshape(-1, 3, d, LANES), (cb, 3, d, LANES), lambda i: (i, 0, 0, 0)
                else:
                    g, block = all_of_0, (cb, side, 1, rows[part], LANES)
                    index = lambda i, part=part: (i % (side // cb), 0, i // (cols // 2), 2 * part + i // (side // cb) % 2, 0)
                so_far = ffn_adam(f, g, block, index, ffn, l, part, PARTS, so_far)
        out = [None] * 21
        for i in range(3):
            for j in range(3):
                out[j * 7 + 4 + i] = so_far[3 * i + j]
        tail = all_of_0[:, :, :, 4 * rows[0] :].reshape(side * side, 2, 2, -1, LANES).transpose(1, 2, 0, 3, 4).reshape(-1, LANES)
        got = small_adam(f, tail[:little_rows].reshape(layers, -1, LANES), [a for i in range(4) for a in (weights[i], m[i], v[i])])
        for i in range(4):
            for j in range(3):
                out[j * 7 + i] = got[3 * i + j]
        return tuple(out)

    states, all_of = P(("rep", "dp"), None, None), P(None, None, None)
    return jax.shard_map(step, mesh=mesh, in_specs=(states, states) + (all_of,) * 21, out_specs=(P("rep", None, None),) * 21, check_vma=False)
```

```python
import functools
import math

import jax
import jax.numpy as jnp
from jax import lax
from jax.experimental import pallas as pl
from jax.experimental.pallas import tpu as pltpu
from jax.sharding import PartitionSpec as P

F32, BF16 = jnp.float32, jnp.bfloat16
LANES = 128
HEAD = 128
THETA = 10000
PARTS = 2
FLAT = (8, LANES)
BQ = 256
LOG2E = 1.4426950408889634
HIDDEN = -1e30
VM = 60 * 2**20


def _nn(a, b):
    return jnp.dot(a, b, preferred_element_type=F32)


def _nt(a, b):
    return lax.dot_general(a, b, (((1,), (1,)), ((), ())), preferred_element_type=F32)


def _whole(*shape):
    return pl.BlockSpec(shape, lambda i: (0,) * len(shape))


def _out(shape, dtype=BF16):
    return jax.ShapeDtypeStruct(shape, dtype)


def _params(*order, **more):
    return pltpu.CompilerParams(dimension_semantics=order or None, vmem_limit_bytes=VM, **more)


HERE = pl.BlockSpec(memory_space=pltpu.VMEM)
UNIT = 2048
ANY = pl.BlockSpec(memory_space=pl.ANY)
ORDER = "arbitrary"
WAYS = (0, 1)
ALL = slice(None)


def _cols(c):
    return slice(c * LANES, (c + 1) * LANES)


def _cost(flops, transcendentals, size):
    return pl.CostEstimate(flops=flops, transcendentals=transcendentals, bytes_accessed=size)


def _peers(n, body, start):
    return lax.fori_loop(1, n, body, start)


def _last():
    return pl.program_id(0) == pl.num_programs(0) - 1


def _norm(h):
    wide = h.astype(F32)
    return wide, lax.rsqrt(jnp.mean(wide * wide, -1, keepdims=True) + 1e-6)


def _norm_back(h, dy, db):
    wide, s = _norm(h)
    dot = jnp.mean(db * wide, -1, keepdims=True)
    return (dy.astype(F32) + s * db - wide * (s * s * s * dot)).astype(BF16)


def _swap(t):
    half = HEAD // 2
    return jnp.concatenate([t[:, half:], t[:, :half]], 1)


def _turn(t, cos, sin):
    t = t.astype(BF16).astype(F32)
    return (t * cos + _swap(t) * sin).astype(BF16)


def _turn_back(t, cos, sin):
    t = t.astype(BF16).astype(F32)
    return (t * cos + _swap(t * sin)).astype(BF16)


def _head(ref, i, rows=ALL):
    return ref[rows, _cols(i)]


def _scores(k, q, at):
    s = _nt(k, q) * (HEAD**-0.5 * LOG2E)
    n = q.shape[0]
    last = s[at:]
    seen = lax.broadcasted_iota(jnp.int32, last.shape, 0) <= lax.broadcasted_iota(jnp.int32, last.shape, 1)
    last = jnp.where(seen, last, HIDDEN)
    return last if at == 0 else jnp.concatenate([s[:at], last], 0)


def _att_fwd(h_ref, wq_ref, wk_ref, wv_ref, wo_ref, cos_ref, sin_ref, y_ref, q_ref, k_ref, v_ref, o_ref, lse_ref):
    cos, sin = cos_ref[...], sin_ref[...]
    wide, s = _norm(h_ref[...])
    a = (wide * s).astype(BF16)
    t, heads = a.shape[0], wq_ref.shape[2] // HEAD
    q = _nn(a, wq_ref[0])
    for i in range(heads):
        q_ref[:, _cols(i)] = _turn(_head(q, i), cos, sin)
    k_ref[...] = _turn(_nn(a, wk_ref[0]), cos, sin)
    v = _nn(a, wv_ref[0]).astype(BF16)
    v_ref[...] = v
    vt = jnp.concatenate([v.T, jnp.ones((16, t), BF16)], 0)
    for at in range(0, t, BQ):
        rows, n = slice(at, at + BQ), at + BQ
        for i in range(heads):
            x = _scores(k_ref[:n, :], _head(q_ref, i, rows), at)
            top = jnp.max(x, 0, keepdims=True)
            p = jnp.exp2(x - top).astype(BF16)
            mix = _nn(vt[:, :n], p)
            total = mix[HEAD : HEAD + 1]
            o_ref[rows, _cols(i)] = (mix[:HEAD] * (1 / total)).T.astype(BF16)
            lse_ref[i : i + 1, rows] = top + jnp.log2(total)
    out = _nn(o_ref[...], wo_ref[0]).astype(BF16)
    y_ref[...] = (h_ref[...].astype(F32) + out.astype(F32)).astype(BF16)


def _att_specs(l, small):
    return [pl.BlockSpec((1, *w.shape[1:]), lambda i: (l, 0, 0)) for w in small]


def att_fwd(h, small, cos, sin, l):
    t, d = h.shape
    wide, narrow = small[0].shape[2], small[1].shape[2]
    heads = wide // HEAD
    shapes = [(t, d), (t, wide), (t, narrow), (t, narrow), (t, wide)]
    return pl.pallas_call(
        _att_fwd, grid=(1,), in_specs=[_whole(t, d), *_att_specs(l, small), _whole(t, HEAD), _whole(t, HEAD)],
        out_specs=[_whole(*s) for s in shapes] + [_whole(heads, t)],
        out_shape=[jax.ShapeDtypeStruct(s, BF16) for s in shapes] + [jax.ShapeDtypeStruct((heads, t), F32)],
        compiler_params=_params(),
        cost_estimate=_cost(4 * t * d * (wide + narrow) + 4 * t * t * wide, t * t * heads, 8 * t * d), name="att_fwd",
    )(h, *small, cos, sin)


def _att_bwd(h_ref, dy_ref, wq_ref, wk_ref, wv_ref, wo_ref, cos_ref, sin_ref, q_ref, k_ref, v_ref, o_ref, lse_ref, dh_ref, g_ref, do_s, dq_s, dk_s, dv_s):
    cos, sin, dy = cos_ref[...], sin_ref[...], dy_ref[...]
    t, heads = dy.shape[0], wq_ref.shape[2] // HEAD
    do_s[...] = _nt(dy, wo_ref[0]).astype(BF16)
    dot = _nt(wo_ref[0], dy).astype(BF16).astype(F32)
    ot = o_ref[...].T
    both = dot * ot.astype(F32)
    deltas = [jnp.sum(both[_cols(i)], 0, keepdims=True) for i in range(heads)]
    at = 0

    def put(g):
        nonlocal at
        g = g.astype(BF16)
        for c in range(0, g.shape[1], LANES):
            g_ref[at : at + g.shape[0], :] = g[:, c : c + LANES]
            at += g.shape[0]

    g_wo = _nn(ot, dy)
    kt = k_ref[...].T
    dk_s[...] = jnp.zeros_like(dk_s)
    dv_s[...] = jnp.zeros_like(dv_s)
    for first in range(0, t, BQ):
        rows, n = slice(first, first + BQ), first + BQ
        for i in range(heads):
            q, do = _head(q_ref, i, rows), _head(do_s, i, rows)
            p = jnp.exp2(_scores(k_ref[:n, :], q, first) - lse_ref[i : i + 1, rows])
            ds = (p * (_nt(v_ref[:n, :], do) - deltas[i][:, rows])).astype(BF16)
            dv_s[:n, :] += _nn(p.astype(BF16), do)
            dk_s[:n, :] += _nn(ds, q)
            dq = (_nn(kt[:, :n], ds) * HEAD**-0.5).T
            dq_s[rows, _cols(i)] = _turn_back(dq, cos[rows], sin[rows])
    dk = _turn_back(dk_s[...] * HEAD**-0.5, cos, sin)
    dv, dq = dv_s[...].astype(BF16), dq_s[...]
    wide, s = _norm(h_ref[...])
    a_t = (wide * s).astype(BF16).T
    put(_nn(a_t, dq))
    put(_nn(a_t, dk))
    put(_nn(a_t, dv))
    put(g_wo)
    g_ref[at:, :] = jnp.zeros((g_ref.shape[0] - at, LANES), BF16)
    da = _nt(dq, wq_ref[0]) + _nt(dk, wk_ref[0]) + _nt(dv, wv_ref[0])
    dh_ref[...] = _norm_back(h_ref[...], dy, da)


def att_bwd(h, dy, small, cos, sin, kept, l):
    t, d = h.shape
    wide, narrow = small[0].shape[2], small[1].shape[2]
    rows = sum(w[0].size for w in small) // LANES
    rows += -rows % UNIT
    return pl.pallas_call(
        _att_bwd, grid=(1,),
        in_specs=[_whole(t, d), _whole(t, d), *_att_specs(l, small), _whole(t, HEAD), _whole(t, HEAD), *(_whole(*a.shape) for a in kept)],
        out_specs=[_whole(t, d), _whole(rows, LANES)],
        out_shape=[jax.ShapeDtypeStruct((t, d), BF16), jax.ShapeDtypeStruct((rows, LANES), BF16)],
        scratch_shapes=[pltpu.VMEM((t, wide), BF16), pltpu.VMEM((t, wide), BF16), pltpu.VMEM((t, narrow), F32), pltpu.VMEM((t, narrow), F32)],
        compiler_params=_params(),
        cost_estimate=_cost(8 * t * d * (wide + narrow) + 10 * t * t * wide, t * t * wide // HEAD, 12 * t * d), name="att_bwd",
    )(h, dy, *small, cos, sin, *kept)


def _ffn_fwd(h_ref, wg_ref, wu_ref, wd_ref, y_ref, *rest, keep):
    (g_ref, u_ref) = rest[:2] if keep else (None, None)
    b_s, y_s = rest[-2:]
    i = pl.program_id(0)
    @pl.when(i == 0)
    def _():
        wide, s = _norm(h_ref[...])
        b_s[...] = (wide * s).astype(BF16)
        y_s[...] = jnp.zeros_like(y_s)
    b = b_s[...]
    gate = _nn(b, wg_ref[0])
    up = _nn(b, wu_ref[0])
    if keep:
        g_ref[...] = gate
        u_ref[...] = up
    hid = (gate * (1 / (1 + jnp.exp(-gate))) * up).astype(BF16)
    y_s[...] += _nn(hid, wd_ref[0])
    @pl.when(_last())
    def _():
        y_ref[...] = (h_ref[...].astype(F32) + y_s[...].astype(BF16).astype(F32)).astype(BF16)

def ffn_fwd(h, wg, wu, wd, l, fc=512, keep=True):
    t, d = h.shape
    ff = wg.shape[2]
    whole = _whole(t, d)
    outs = [jax.ShapeDtypeStruct((t, d), BF16)]
    ospecs = [whole]
    if keep:
        outs += [jax.ShapeDtypeStruct((t, ff), F32)] * 2
        ospecs += [pl.BlockSpec((t, fc), lambda i: (0, i))] * 2
    return pl.pallas_call(
        functools.partial(_ffn_fwd, keep=keep), grid=(ff // fc,),
        in_specs=[whole, pl.BlockSpec((1, d, fc), lambda i: (l, 0, i)), pl.BlockSpec((1, d, fc), lambda i: (l, 0, i)),
                  pl.BlockSpec((1, fc, d), lambda i: (l, i, 0))],
        out_specs=ospecs, out_shape=outs,
        scratch_shapes=[pltpu.VMEM((t, d), BF16), pltpu.VMEM((t, d), F32)],
        compiler_params=_params(ORDER),
        cost_estimate=_cost(6 * t * d * ff, t * ff, 3 * d * ff * 2), name="ffn_fwd",
    )(h, wg, wu, wd)

def _ffn_bwd(*refs, saved):
    refs = list(refs)
    h_ref, dy_ref, wg_ref, wu_ref, wd_ref = refs[:5]
    refs = refs[5:]
    if saved:
        g_ref, u_ref = refs[:2]
        refs = refs[2:]
    G_ref, db_ref, b_s, bT_s, dyT_s, db_s = refs
    i = pl.program_id(0)
    @pl.when(i == 0)
    def _():
        wide, s = _norm(h_ref[...])
        b = (wide * s).astype(BF16)
        b_s[...] = b
        bT_s[...] = b.T
        dyT_s[...] = dy_ref[...].T
        db_s[...] = jnp.zeros_like(db_s)
    b, dy = b_s[...], dy_ref[...]
    wg, wu, wd = wg_ref[0], wu_ref[0], wd_ref[0]
    fc = wg.shape[1]
    if saved:
        gate, up = g_ref[...], u_ref[...]
    else:
        gate, up = _nn(b, wg), _nn(b, wu)
    dhid = _nt(dy, wd).astype(BF16).astype(F32)
    sig = 1 / (1 + jnp.exp(-gate))
    act = gate * sig
    hid = (act * up).astype(BF16)
    dup = (dhid * act).astype(BF16)
    dgate = (dhid * up * (sig * (1 + gate * (1 - sig)))).astype(BF16)
    db_s[...] += _nt(dgate, wg) + _nt(dup, wu)
    bT, dyT = bT_s[...], dyT_s[...]
    for k, (x, z) in enumerate(((bT, dgate), (bT, dup), (dyT, hid))):
        w = _nn(x, z).astype(BF16)
        for c in range(fc // LANES):
            G_ref[c, k] = w[:, _cols(c)]
    @pl.when(_last())
    def _():
        db_ref[...] = _norm_back(h_ref[...], dy_ref[...], db_s[...])


def ffn_bwd(h, dy, wg, wu, wd, l, fc=512, kept=None):
    t, d = h.shape
    ff = wg.shape[2]
    whole = _whole(t, d)
    col = pl.BlockSpec((1, d, fc), lambda i: (l, 0, i))
    args, specs = [h, dy, wg, wu, wd], [whole, whole, col, col, pl.BlockSpec((1, fc, d), lambda i: (l, i, 0))]
    if kept:
        args += list(kept)
        specs += [pl.BlockSpec((t, fc), lambda i: (0, i))] * 2
    return pl.pallas_call(
        functools.partial(_ffn_bwd, saved=bool(kept)), grid=(ff // fc,),
        in_specs=specs,
        out_specs=[pl.BlockSpec((fc // LANES, 3, d, LANES), lambda i: (i, 0, 0, 0)), whole],
        out_shape=[_out((ff // LANES, 3, d, LANES)), _out((t, d))],
        scratch_shapes=[pltpu.VMEM((t, d), BF16), pltpu.VMEM((d, t), BF16), pltpu.VMEM((d, t), BF16), pltpu.VMEM((t, d), F32)],
        compiler_params=_params(ORDER), cost_estimate=_cost(16 * t * d * ff, t * ff, 12 * d * ff), name="ffn_bwd",
    )(*args)


def _adam(w, m, v, g):
    m = 0.9 * m + 0.1 * g
    v = 0.95 * v + 0.05 * g * g
    return (w.astype(F32) - 0.02 * (m * lax.rsqrt(v + 1e-8) + 0.1 * w.astype(F32))).astype(BF16), m, v


def _ffn_adam(f_ref, g_ref, *refs):
    ins, outs = refs[:9], refs[-9:]
    f = f_ref[0:1, 0:1]
    d, cb = ins[0].shape[1], ins[0].shape[2] // LANES
    for c in range(cb):
        at = _cols(c)
        rows = g_ref[c].reshape(3 * d, LANES)
        for k in range(3):
            g = rows[k * d : (k + 1) * d].astype(F32) * f
            where = (0, ALL, at)
            if k == 2:
                g, where = g.T, (0, at, ALL)
            got = _adam(*(r[where] for r in ins[3 * k : 3 * k + 3]), g)
            for r, x in zip(outs[3 * k : 3 * k + 3], got):
                r[where] = x


def ffn_adam(f, g, block, index, arrays, l, so_far, cb):
    _, d, ff = arrays[0].shape
    wide = pl.BlockSpec((1, d, cb * LANES), lambda i: (l, 0, i))
    tall = pl.BlockSpec((1, cb * LANES, d), lambda i: (l, i, 0))
    specs = [wide] * 6 + [tall] * 3
    chain = list(so_far or ())
    return pl.pallas_call(
        _ffn_adam, grid=(ff // LANES // cb,),
        in_specs=[_whole(*f.shape), pl.BlockSpec(block, index)] + specs + [ANY] * len(chain),
        out_specs=specs, out_shape=[jax.ShapeDtypeStruct(a.shape, a.dtype) for a in arrays],
        input_output_aliases={11 + i: i for i in range(len(chain))},
        compiler_params=_params(ORDER), cost_estimate=_cost(6000 * d * ff, 3 * d * ff, 66 * d * ff), name="ffn_adam",
    )(f, g, *arrays, *chain)


def _small_adam(f_ref, a_ref, b_ref, *refs):
    x, y, cores, _, _ = a_ref.shape
    g_ref = jnp.concatenate([r[i, j, core] for core in range(cores) for r in (a_ref, b_ref) for i in range(x) for j in range(y)])
    ins, outs = refs[: len(refs) // 2], refs[len(refs) // 2 :]
    f, at = f_ref[0:1, 0:1], 0
    for k in range(len(ins) // 3):
        _, rows, cols = ins[3 * k].shape
        for c in range(cols // LANES):
            where = (0, ALL, _cols(c))
            g = g_ref[at : at + rows].astype(F32) * f
            at += rows
            got = _adam(*(r[where] for r in ins[3 * k : 3 * k + 3]), g)
            for r, x in zip(outs[3 * k : 3 * k + 3], got):
                r[where] = x


def small_adam(f, g, piece, first, arrays):
    specs = [pl.BlockSpec((1, *a.shape[1:]), lambda i: (i, 0, 0)) for a in arrays]
    block = (*g.shape[:3], piece, LANES)
    size = sum(a.size for a in arrays)
    return pl.pallas_call(
        _small_adam, grid=(arrays[0].shape[0],),
        in_specs=[_whole(*f.shape)] + [pl.BlockSpec(block, lambda i, p=p: (0, 0, 0, first + 2 * i + p, 0)) for p in WAYS] + specs,
        out_specs=specs, out_shape=[jax.ShapeDtypeStruct(a.shape, a.dtype) for a in arrays],
        compiler_params=_params(ORDER), cost_estimate=_cost(700 * size, size, 8 * size), name="small_adam",
    )(f, g, g, *arrays)


def _factor(x_ref, f_ref, all_s, send, recv, *, axis, n, count):
    me = lax.axis_index(axis)
    barrier = pltpu.get_barrier_semaphore()

    def peer(i):
        return lax.rem(me + i, n)

    def greet(i, _):
        pl.semaphore_signal(barrier, inc=1, device_id={axis: peer(i)}, device_id_type=pl.DeviceIdType.MESH)

    _peers(n, greet, None)
    pl.semaphore_wait(barrier, n - 1)

    def copy(i):
        return pltpu.make_async_remote_copy(src_ref=x_ref, dst_ref=all_s.at[i], send_sem=send.at[i], recv_sem=recv.at[i],
                                            device_id={axis: peer(i)}, device_id_type=pl.DeviceIdType.MESH)

    _peers(n, lambda i, _: copy(i).start(), None)
    _peers(n, lambda i, _: copy(i).wait(), None)
    total = x_ref[...]
    total = _peers(n, lambda i, t: t + all_s[i], total)
    total = jnp.sum(jnp.sum(total, 0, keepdims=True), 1, keepdims=True)
    f_ref[...] = jnp.broadcast_to(jnp.minimum(1.0, 0.5 * lax.rsqrt(total / count + 1e-30)), f_ref.shape)


def factor(x, axis, n, count):
    return pl.pallas_call(
        functools.partial(_factor, axis=axis, n=n, count=count),
        in_specs=[HERE], out_specs=HERE,
        out_shape=jax.ShapeDtypeStruct(x.shape, F32),
        scratch_shapes=[pltpu.VMEM((n, *x.shape), F32), pltpu.SemaphoreType.DMA((n,)), pltpu.SemaphoreType.DMA((n,))],
        compiler_params=pltpu.CompilerParams(collective_id=0, has_side_effects=True),
        cost_estimate=_cost(10**7, 0, 10**6), name="factor",
    )(x)


def _scatter(*refs, axis, rows, side, places, arrays):
    (out_ref, *rest) = refs[arrays:]
    units, bases = [refs[i] for i, _ in places], [at for _, at in places]
    bufs, sems = rest[: 9 * len(rows)], rest[9 * len(rows) :]
    own_sem, p0s, p0r, s1s, s1r, s2s, s2r, t1s, t1r, t2s, t2r = sems
    me = lax.axis_index(axis)
    core, x, y = lax.rem(me, 2), lax.div(me, 2 * side), lax.rem(lax.div(me, 2), side)
    device = lambda x, y, core: {axis: (x * side + y) * 2 + core}
    ring = lambda n: lax.rem(n + 2 * side, side)
    partner = device(x, y, 1 - core)
    near = [[device(ring(x + 1), y, core), device(ring(x - 1), y, core)], [device(x, ring(y + 1), core), device(x, ring(y - 1), core)]]
    barrier = pltpu.get_barrier_semaphore()
    for to in [partner, *near[0], *near[1]]:
        pl.semaphore_signal(barrier, inc=1, device_id=to, device_id_type=pl.DeviceIdType.MESH)
    pl.semaphore_wait(barrier, 5)
    flows = [(u, p) for u in range(len(rows)) for p in WAYS]
    left_over = []
    piece_of, chunk_of = (lambda u: rows[u] // 64), (lambda u: rows[u] // 16)

    def send(src, dst, s, r, to):
        copy = pltpu.make_async_remote_copy(src_ref=src, dst_ref=dst, send_sem=s, recv_sem=r, device_id=to, device_id_type=pl.DeviceIdType.MESH)
        copy.start()
        left_over.append(copy)

    def add(n, outs, *ins):
        step = max(b for b in (256, 240, 128, 112, 64) if n % b == 0)

        def body(i, _):
            total = None
            for ref, at in ins:
                t = ref[pl.ds(pl.multiple_of(at + i * step, 16), step), :].astype(F32)
                total = t if total is None else total + t
            for ref, at in outs:
                ref[pl.ds(pl.multiple_of(at + i * step, 16), step), :] = total.astype(ref.dtype)

        lax.fori_loop(0, n // step, body, None)

    own = lambda u: bufs[9 * u]
    other = lambda u: bufs[9 * u + 1]
    (A1, R1, A2, R2, MID, B1, Q1) = (lambda u, i=i: bufs[9 * u + 2 + i] for i in range(7))
    place = lambda p: (x, y)[p]
    cross = lambda p: (y, x)[p]
    chunk = lambda u, p, j: p * (rows[u] // 4) + j * (chunk_of(u))

    def fetch(u, p, j, half):
        piece, base = piece_of(u), bases[u] + half * (rows[u] // 2) + p * (rows[u] // 4)
        if p == 0:
            return [(base + j * (chunk_of(u)), chunk(u, p, j), chunk_of(u))]
        return [(base + (i * side + j) * piece, chunk(u, p, j) + i * piece, piece) for i in range(side)]

    al = lambda n: pl.multiple_of(n, 16)
    at_of = lambda ref, a, n: ref.at[pl.ds(al(a), n), :]
    for f, (u, p) in enumerate(flows):
        for k in (2, 1, 3, 0):
            j = ring(place(p) + k)
            for src, dst, n in fetch(u, p, j, 1 - core):
                copy = pltpu.make_async_remote_copy(src_ref=at_of(units[u], src, n), dst_ref=at_of(other(u), dst, n), send_sem=p0s.at[f, k],
                                                    recv_sem=p0r.at[f, k], device_id=partner, device_id_type=pl.DeviceIdType.MESH)
                copy.start()
            for src, dst, n in fetch(u, p, j, core):
                pltpu.make_async_copy(at_of(units[u], src, n), at_of(own(u), dst, n), own_sem.at[f, k]).start()

    def arrived(f, k):
        u, p = flows[f]
        a, n = chunk(u, p, ring(place(p) + k)), chunk_of(u)
        pltpu.make_async_copy(at_of(own(u), a, n), at_of(own(u), a, n), own_sem.at[f, k]).wait()
        pltpu.make_async_remote_copy(src_ref=at_of(other(u), a, n), dst_ref=at_of(other(u), a, n), send_sem=p0s.at[f, k], recv_sem=p0r.at[f, k],
                                     device_id=partner, device_id_type=pl.DeviceIdType.MESH).wait()
        return a

    def landed(ref, a, n, f, i, sem_s, sem_r, to):
        pltpu.make_async_remote_copy(src_ref=ref.at[pl.ds(a, n), :], dst_ref=ref.at[pl.ds(a, n), :], send_sem=sem_s.at[f, i], recv_sem=sem_r.at[f, i],
                                     device_id=to, device_id_type=pl.DeviceIdType.MESH).wait_recv()

    def one(f):
        u, p = flows[f]
        n = chunk_of(u) // 2
        a = arrived(f, 2)
        add(2 * n, [(A1(u), 2 * p * n)], (own(u), a), (other(u), a))
        for way in WAYS:
            at = (2 * p + way) * n
            send(A1(u).at[pl.ds(at, n), :], R1(u).at[pl.ds(at, n), :], s1s.at[f, way], s1r.at[f, way], near[p][way])

    def two(f):
        u, p = flows[f]
        n = chunk_of(u) // 2
        for way in WAYS:
            a = arrived(f, (1, 3)[way])
            landed(R1(u), (2 * p + way) * n, n, f, way, s1s, s1r, near[p][way])
            at = (2 * p + way) * 2 * n
            with_, plain = way * n, (1 - way) * n
            add(n, [(A2(u), at + with_)], (own(u), a + with_), (other(u), a + with_), (R1(u), (2 * p + way) * n))
            add(n, [(A2(u), at + plain)], (own(u), a + plain), (other(u), a + plain))
            send(A2(u).at[pl.ds(at, 2 * n), :], R2(u).at[pl.ds(at, 2 * n), :], s2s.at[f, way], s2r.at[f, way], near[p][way])

    def three(f):
        u, p = flows[f]
        n, piece = chunk_of(u), piece_of(u)
        a = arrived(f, 0)
        for way in WAYS:
            landed(R2(u), (2 * p + way) * n, n, f, way, s2s, s2r, near[p][way])
        add(n, [(MID(u), p * n)], (own(u), a), (other(u), a), (R2(u), 2 * p * n), (R2(u), (2 * p + 1) * n))
        far = p * n + ring(cross(p) + 2) * piece
        at = p * 3 * piece
        add(piece, [(B1(u), at)], (MID(u), far))
        for way in WAYS:
            here = pl.ds(at + way * (piece // 2), piece // 2)
            send(B1(u).at[here, :], Q1(u).at[here, :], t1s.at[f, way], t1r.at[f, way], near[1 - p][way])

    def four(f):
        u, p = flows[f]
        n, piece = chunk_of(u), piece_of(u)
        for way in WAYS:
            first = 3 * p * piece
            landed(Q1(u), first + way * (piece // 2), piece // 2, f, way, t1s, t1r, near[1 - p][way])
            src = p * n + ring(cross(p) + (1, 3)[way]) * piece
            at = first + (1 + way) * piece
            with_, plain = way * (piece // 2), (1 - way) * (piece // 2)
            add(piece // 2, [(B1(u), at + with_)], (MID(u), src + with_), (Q1(u), first + way * (piece // 2)))
            add(piece // 2, [(B1(u), at + plain)], (MID(u), src + plain))
            send(B1(u).at[pl.ds(at, piece), :], Q1(u).at[pl.ds(at, piece), :], t2s.at[f, way], t2r.at[f, way], near[1 - p][way])

    def five(f):
        u, p = flows[f]
        n, piece = chunk_of(u), piece_of(u)
        first = 3 * p * piece
        for way in WAYS:
            landed(Q1(u), first + (1 + way) * piece, piece, f, way, t2s, t2r, near[1 - p][way])
        add(piece, [(out_ref, sum(r // 32 for r in rows[:u]) + p * piece)], (MID(u), p * n + ring(cross(p)) * piece),
            (Q1(u), first + piece), (Q1(u), first + 2 * piece))

    stages = (one, two, three, four, five)
    for t in range(len(flows) + 2 * (len(stages) - 1)):
        for k, stage in enumerate(stages):
            if 0 <= t - 2 * k < len(flows):
                stage(t - 2 * k)
    for copy in left_over:
        copy.wait_send()


def ring_scatter(units, axis, side, most):
    places = [(i, at) for i, u in enumerate(units) for at in range(0, u.shape[0], most)]
    rows = tuple(min(units[i].shape[0], most) for i, _ in places)
    buf = lambda n, t=BF16: pltpu.VMEM((n, LANES), t)
    scratch = []
    for r in rows:
        scratch += [buf(r // 2), buf(r // 2), buf(r // 8), buf(r // 8), buf(r // 4), buf(r // 4), buf(r // 8, F32), buf(3 * r // 32), buf(3 * r // 32)]
    f = 2 * len(rows)
    total = sum(rows)
    return pl.pallas_call(
        functools.partial(_scatter, axis=axis, rows=rows, side=side, places=places, arrays=len(units)),
        in_specs=[ANY] * len(units), out_specs=HERE,
        out_shape=jax.ShapeDtypeStruct((total // 32, LANES), BF16),
        scratch_shapes=scratch + [pltpu.SemaphoreType.DMA((f, 4))] * 3 + [pltpu.SemaphoreType.DMA((f, 2))] * 8,
        compiler_params=_params(collective_id=1, has_side_effects=True),
        cost_estimate=_cost(5 * 10**10, 0, total * LANES * 2), name="ring_scatter",
    )(*units)


def solution(mesh):
    n = mesh.shape["dp"]

    def step(x, dy, *arrays):
        weights, m, v = (arrays[i : i + 7] for i in (0, 7, 14))
        layers, d, ff = weights[4].shape
        small, (wg, wu, wd) = weights[:4], weights[4:]
        count = sum(w.size for w in weights)
        h = x[0]
        half = HEAD // 2
        angle = jnp.arange(h.shape[0], dtype=F32)[:, None] * THETA ** (-jnp.arange(half, dtype=F32) / half)
        cos, sin = jnp.cos(angle), jnp.sin(angle)
        cos, sin = jnp.concatenate([cos, cos], 1), jnp.concatenate([-sin, sin], 1)
        kept, backs = [], []
        for l in range(layers):
            y, *rest = att_fwd(h, small, cos, sin, l)
            backs.append((h, rest))
            h = y
            if l < layers - 1:
                y, *gu = ffn_fwd(h, wg, wu, wd, l)
                kept.append((h, gu))
                h = y
            else:
                kept.append((h, None))
        by_h = dy[0]
        side = math.isqrt(n // 2)
        summed, little = {}, {}
        add_up = lambda s: jnp.sum(jnp.square(s.astype(F32)).reshape(-1, *FLAT), 0)
        for l in reversed(range(layers)):
            at_ffn, gu = kept[l]
            g, by_h = ffn_bwd(at_ffn, by_h, wg, wu, wd, l, kept=gu)
            big = g.reshape(-1, LANES)
            if l:
                summed[l] = lax.psum(big, "dp")
            before, rest = backs[l]
            by_h, little[l] = att_bwd(before, by_h, small, cos, sin, rest, l)
        most = big.shape[0] // PARTS
        shard = ring_scatter([big, *(little[l] for l in range(layers))], "dp", side, most)
        me = lax.axis_index("dp")
        squares = add_up(shard)
        for s in summed.values():
            rows = s.shape[0] // n
            squares += add_up(lax.dynamic_slice_in_dim(s, me * rows, rows))
        f = factor(squares, "dp", n, count)
        all_of_0 = lax.all_gather(shard, "dp", axis=0, tiled=True).reshape(side, side, 2, -1, LANES)
        ffn = [a for i in (4, 5, 6) for a in (weights[i], m[i], v[i])]
        so_far, cb = None, 4
        cols, across = ff // PARTS // LANES // cb, side // cb
        for l in reversed(range(layers)):
            if l:
                g, block, index = summed[l].reshape(-1, 3, d, LANES), (cb, 3, d, LANES), lambda i: (i, 0, 0, 0)
            else:
                g, block = all_of_0, (cb, side, 1, most // 64, LANES)
                index = lambda i: (i % across, 0, i % cols // (cols // 2), 2 * (i // cols) + i // across % 2, 0)
            so_far = ffn_adam(f, g, block, index, ffn, l, so_far, cb)
        piece = little[0].shape[0] // 64
        got = small_adam(f, all_of_0, piece, big.shape[0] // n // piece, [a for i in range(4) for a in (weights[i], m[i], v[i])])
        out = [*got[::3], *so_far[::3], *got[1::3], *so_far[1::3], *got[2::3], *so_far[2::3]]
        return tuple(out)

    states, all_of = P(("rep", "dp"), None, None), P(None, None, None)
    return jax.shard_map(step, mesh=mesh, in_specs=(states, states) + (all_of,) * 21, out_specs=(P("rep", None, None),) * 21, check_vma=False)
```
